32 devices in a mesh: groups: 2 (over x), seq: 16 (over z, y, core).
Axes of the slice: x: 2, y: 2, z: 4, core: 2. Of those that a mesh axis runs over, the one named last changes fastest.
Arguments:
- latent_noise: float32 [4096, 192], P(('groups', 'seq')), parts along dimension 0, may hold values from -6 to 6
- position: bfloat16 [2048, 768], P('seq'), may hold values from -2 to 2
- in_weight: bfloat16 [192, 768], replicated, may hold values from -0.4375 to 0.4375
- gain_attn: float32 [768], replicated, may hold values from 0.1 to 1.9
- query_weight: bfloat16 [768, 384], replicated, may hold values from -5.1 to 5.1
- key_weight: bfloat16 [768, 384], replicated, may hold values from -5.1 to 5.1
- value_weight: bfloat16 [768, 384], replicated, may hold values from -0.21875 to 0.21875
- mix_weight: bfloat16 [384, 768], replicated, may hold values from -0.3125 to 0.3125
- gain_mlp: float32 [768], replicated, may hold values from 0.1 to 1.9
- up_weight: bfloat16 [768, 1536], replicated, may hold values from -0.21875 to 0.21875
- down_weight: bfloat16 [1536, 768], replicated, may hold values from -0.15625 to 0.15625
- gain_out: float32 [768], replicated, may hold values from 0.1 to 1.9
- out_weight: bfloat16 [768, 384], replicated, may hold values from -0.15625 to 0.15625
Outputs:
- sample: float32 [4096, 192], P(('groups', 'seq')), parts along dimension 0
The draws below stay inside these ranges and needn't reach their ends.
There are 2 independent parts, one for each index of `groups`. The reference program is written for one: setup_inputs(seed, part) draws one part's arguments, and reference() takes and returns one part's arrays. A program takes and returns all parts, laid end to end along the dimension named above; an argument that names none is the same for every part. Nothing has to cross between parts.
All inputs are finite; a program needn't handle non-finite values.
Results may differ from the reference program's by a relative error of at most 0.04.
Values may be sent and summed in bfloat16 or wider, within the bound.
No kernel may reach another device: no remote copies, remote signals or barrier semaphores. Data moves between devices by JAX's collectives and lax.ppermute only.
A program may use at most 128 MiB of HBM per device.

```python
import math
import jax
import jax.numpy as jnp
from jax import lax

PATCH = 192
D = 768
HEADS = 6
HD = 64
FF = 1536
ITERS = 2
SEQ = 2048


def paired_projections(key):
    base_key = jax.random.fold_in(key, 7301)
    other_key = jax.random.fold_in(key, 7302)
    base = jnp.clip(jax.random.normal(base_key, (D, HEADS * HD), jnp.float32), -4.0, 4.0)
    other = jnp.clip(jax.random.normal(other_key, (D, HEADS * HD), jnp.float32), -4.0, 4.0)
    factor = 2.0 / math.sqrt(D)
    return (base * factor, other * factor)


def draw_query_weight(key, part):
    return paired_projections(key)[0].astype(jnp.bfloat16)


def draw_key_weight(key, part):
    return paired_projections(key)[1].astype(jnp.bfloat16)


def block_scale(rng, dims, cuts, low, largest):
    level, own = 1.0, jax.random.fold_in(rng, 6)
    for dim, parts in cuts:
        steps = jnp.exp(jax.random.uniform(jax.random.fold_in(own, dim), (parts,), jnp.float32, low / len(cuts), largest / len(cuts)))
        level = level * jnp.repeat(steps, dims[dim] // parts).reshape([-1 if axis == dim else 1 for axis in range(len(dims))])
    return level


def normal_values(key, dims, width, reach, shards=(), kind=jnp.bfloat16):
    result = width * jax.random.normal(key, dims, jnp.float32)
    if shards:
        result = result * block_scale(key, dims, shards, -0.22, 0.18)
    return jnp.clip(result, -reach, reach).astype(kind)


def setup_inputs(seed: int = 0, part: int = 0) -> dict:
    keys = jax.random.split(jax.random.key(seed), 14)
    part_keys = jax.random.split(jax.random.fold_in(keys[13], part), 14)
    return {
        "latent_noise": normal_values(part_keys[0], (SEQ, PATCH), 1.0, 6.0, ((0, 16),), jnp.float32),
        "position": normal_values(keys[1], (SEQ, D), 0.25, 2.0, ((0, 16),)),
        "in_weight": normal_values(keys[2], (PATCH, D), PATCH ** -0.5, 0.4375),
        "gain_attn": jnp.clip(1.0 + 0.18 * jax.random.normal(keys[3], (D,), jnp.float32), 0.1, 1.9),
        "query_weight": draw_query_weight(jax.random.fold_in(keys[13], 71), part),
        "key_weight": draw_key_weight(jax.random.fold_in(keys[13], 71), part),
        "value_weight": normal_values(keys[6], (D, HEADS * HD), D ** -0.5, 0.21875),
        "mix_weight": normal_values(keys[7], (HEADS * HD, D), (HEADS * HD) ** -0.5, 0.3125),
        "gain_mlp": jnp.clip(1.0 + 0.18 * jax.random.normal(keys[8], (D,), jnp.float32), 0.1, 1.9),
        "up_weight": normal_values(keys[9], (D, FF), D ** -0.5, 0.21875),
        "down_weight": normal_values(keys[10], (FF, D), FF ** -0.5, 0.15625),
        "gain_out": jnp.clip(1.0 + 0.18 * jax.random.normal(keys[11], (D,), jnp.float32), 0.1, 1.9),
        "out_weight": normal_values(keys[12], (D, 2 * PATCH), (2 * D) ** -0.5, 0.15625),
    }


def rms_norm(values, gain):
    scale = lax.rsqrt(lax.optimization_barrier(jnp.mean(values * values, axis=-1, keepdims=True)) + 1e-06)
    return values * scale * gain

def attend(query_rows, key_rows, value_rows):
    block_rows = math.gcd(SEQ, 512)
    pieces = []
    for first_row in range(0, SEQ, block_rows):
        end_row = first_row + block_rows
        query_heads = query_rows[first_row:end_row].astype(jnp.float32).reshape(block_rows, HEADS, HD)
        key_heads = key_rows[:end_row].astype(jnp.float32).reshape(end_row, HEADS, HD)
        value_heads = value_rows[:end_row].astype(jnp.float32).reshape(end_row, HEADS, HD)
        scores = jnp.einsum('qhd,khd->hqk', query_heads, key_heads, precision=lax.Precision.HIGHEST) * HD ** (-0.5)
        query_pos = first_row + jnp.arange(block_rows, dtype=jnp.int32)
        key_pos = jnp.arange(end_row, dtype=jnp.int32)
        causal = (key_pos[None, :] <= query_pos[:, None])[None]
        masked = jnp.where(causal, scores, -1e+30)
        row_max = lax.optimization_barrier(jnp.max(masked, axis=2, keepdims=True))
        weights = jnp.where(causal, jnp.exp(masked - row_max), 0.0)
        totals = lax.optimization_barrier(jnp.sum(weights, axis=2, keepdims=True))
        rounded = weights.astype(jnp.bfloat16).astype(jnp.float32)
        attended = jnp.einsum('hqk,khd->hqd', rounded, value_heads, precision=lax.Precision.HIGHEST) / totals
        pieces.append(jnp.transpose(attended, (1, 0, 2)).reshape(block_rows, HEADS * HD))
    return jnp.concatenate(pieces, axis=0).astype(jnp.bfloat16)

def jacobi_step(current, latent_noise, position, in_weight, gain_attn, query_weight, key_weight, value_weight, mix_weight, gain_mlp, up_weight, down_weight, gain_out, out_weight):
    shifted = jnp.concatenate([jnp.zeros((1, PATCH), current.dtype), current[:-1]], axis=0)
    hidden_in = jnp.dot(shifted.astype(jnp.bfloat16), in_weight, preferred_element_type=jnp.float32) + position.astype(jnp.float32)
    normed_attn = rms_norm(hidden_in, gain_attn).astype(jnp.bfloat16)
    query_rows = jnp.dot(normed_attn, query_weight, preferred_element_type=jnp.float32).astype(jnp.bfloat16)
    key_rows = jnp.dot(normed_attn, key_weight, preferred_element_type=jnp.float32).astype(jnp.bfloat16)
    value_rows = jnp.dot(normed_attn, value_weight, preferred_element_type=jnp.float32).astype(jnp.bfloat16)
    attended = attend(query_rows, key_rows, value_rows)
    hidden_mid = hidden_in + jnp.dot(attended, mix_weight, preferred_element_type=jnp.float32)
    normed_mlp = rms_norm(hidden_mid, gain_mlp).astype(jnp.bfloat16)
    activated = jax.nn.gelu(jnp.dot(normed_mlp, up_weight, preferred_element_type=jnp.float32)).astype(jnp.bfloat16)
    hidden_out = hidden_mid + jnp.dot(activated, down_weight, preferred_element_type=jnp.float32)
    normed_out = rms_norm(hidden_out, gain_out).astype(jnp.bfloat16)
    statistics = jnp.dot(normed_out, out_weight, preferred_element_type=jnp.float32)
    mean_shift = statistics[:, :PATCH]
    log_scale = statistics[:, PATCH:]
    return latent_noise * jnp.exp(log_scale) + mean_shift

def reference(latent_noise, position, in_weight, gain_attn, query_weight, key_weight, value_weight, mix_weight, gain_mlp, up_weight, down_weight, gain_out, out_weight):
    current = latent_noise
    for iteration in range(ITERS):
        current = jacobi_step(current, latent_noise, position, in_weight, gain_attn, query_weight, key_weight, value_weight, mix_weight, gain_mlp, up_weight, down_weight, gain_out, out_weight)
    return current[::-1]
```

```python
import functools

import jax
import jax.numpy as jnp
from jax import lax
from jax.experimental import pallas as pl
from jax.experimental.pallas import tpu as pltpu
from jax.sharding import PartitionSpec as P

HEADS = 6
GROUP = 3
EPS = 1e-06
F32, BF16 = jnp.float32, jnp.bfloat16

VM = pl.BlockSpec(memory_space=pltpu.VMEM)
SM = pl.BlockSpec(memory_space=pltpu.SMEM)
HB = pl.BlockSpec(memory_space=pltpu.HBM)


def dot(a, b):
    return jnp.dot(a, b, preferred_element_type=F32)


def norm_scale(values):
    return lax.rsqrt(jnp.mean(values * values, axis=-1, keepdims=True) + EPS)


def pick(flag, left, right):
    return jnp.where(flag, left, right)


def shifted_down(values, first_row):
    rows = lax.broadcasted_iota(jnp.int32, values.shape, 0)
    return jnp.where(rows == 0, first_row, pltpu.roll(values, 1, 0))


def shifted_up(values, last_row):
    count = values.shape[0]
    rows = lax.broadcasted_iota(jnp.int32, values.shape, 0)
    return jnp.where(rows == count - 1, last_row, pltpu.roll(values, count - 1, 0))


def project(ids, normed, wq_ref, wk_ref, wv_ref, scale):
    even = ids[0] == 0
    half = wq_ref.shape[1] // 2
    query = (dot(normed, wq_ref[...]).astype(BF16) * scale).astype(BF16)
    key = dot(normed, wk_ref[...]).astype(BF16)
    value = dot(normed, wv_ref[...]).astype(BF16)
    left = jnp.concatenate([key[:, :half], value[:, :half]], axis=1)
    right = jnp.concatenate([key[:, half:], value[:, half:]], axis=1)
    return query, pick(even, left, right), pick(even, right, left)


def prologue(ids, z_ref, halo_ref, pos_ref, win_ref, gain_ref, wq_ref, wk_ref, wv_ref, h_ref, q_ref, own_ref, oth_ref):
    x = shifted_down(z_ref[...], halo_ref[...].astype(F32))
    hidden = dot(x.astype(BF16), win_ref[...]) + pos_ref[...].astype(F32)
    normed = (hidden * norm_scale(hidden) * gain_ref[...]).astype(BF16)
    scale = (wq_ref.shape[1] // HEADS) ** (-0.5)
    query, own, oth = project(ids, normed, wq_ref, wk_ref, wv_ref, scale)
    h_ref[...] = hidden
    q_ref[...] = query
    own_ref[...] = own
    oth_ref[...] = oth


def change_map(ids, win_ref, gain_ref, wk_ref, wv_ref, a_ref):
    even = ids[0] == 0
    half = wk_ref.shape[1] // 2
    scaled = (win_ref[...].astype(F32) * gain_ref[...]).astype(BF16)
    key = dot(scaled, wk_ref[...]).astype(BF16)
    value = dot(scaled, wv_ref[...]).astype(BF16)
    left = jnp.concatenate([key[:, :half], value[:, :half]], axis=1)
    right = jnp.concatenate([key[:, half:], value[:, half:]], axis=1)
    a_ref[...] = jnp.concatenate([pick(even, left, right), pick(even, right, left)], axis=1)


def attend_half(query_half, pieces, starts, query_base, s_ref, p_ref, pass_heads):
    rows, width = query_half.shape
    head = width // GROUP
    lane_head = lax.broadcasted_iota(jnp.int32, (rows, width), 1) // head
    row_id = query_base + lax.broadcasted_iota(jnp.int32, (rows, rows), 0)
    lane_id = lax.broadcasted_iota(jnp.int32, (rows, rows), 1)
    diff = row_id - lane_id
    result = jnp.zeros((rows, width), F32)
    for first in range(0, GROUP, pass_heads):
        heads = range(first, first + pass_heads)
        stacked = jnp.concatenate([jnp.where(lane_head == i, query_half, jnp.zeros_like(query_half)) for i in heads], axis=0)
        top = jnp.full((pass_heads * rows, rows), -1e30, F32)
        for j, piece in enumerate(pieces):
            scores = lax.dot_general(stacked, piece[:, :width], (((1,), (1,)), ((), ())), preferred_element_type=F32)
            for part in range(2):
                keep = diff >= starts[j][part]
                block = scores[:, part * rows : (part + 1) * rows]
                block = jnp.concatenate(
                    [jnp.where(keep, block[i * rows : (i + 1) * rows], -1e30) for i in range(pass_heads)], axis=0
                )
                top = jnp.maximum(top, block)
                s_ref[:, pl.ds((2 * j + part) * rows, rows)] = block
        row_max = jnp.max(top, axis=1, keepdims=True)
        total = jnp.zeros((pass_heads * rows, rows), F32)
        for j in range(2 * len(pieces)):
            weight = jnp.exp(s_ref[:, pl.ds(j * rows, rows)] - row_max)
            total = total + weight
            p_ref[:, pl.ds(j * rows, rows)] = weight.astype(BF16)
        product = jnp.zeros((pass_heads * rows, width), F32)
        for j, piece in enumerate(pieces):
            product = product + dot(p_ref[:, pl.ds(2 * j * rows, 2 * rows)], piece[:, width : 2 * width])
        product = product / jnp.sum(total, axis=1, keepdims=True)
        for k, i in enumerate(heads):
            result = result + jnp.where(lane_head == i, product[k * rows : (k + 1) * rows], 0.0)
    return result.astype(BF16)


def finish_step(hidden, attended, latent, mix_ref, gmlp_ref, up_ref, down_ref, gout_ref, out_ref):
    patch = latent.shape[1]
    mid = hidden + dot(attended, mix_ref[...])
    normed = (mid * norm_scale(mid) * gmlp_ref[...]).astype(BF16)
    active = jax.nn.gelu(dot(normed, up_ref[...])).astype(BF16)
    final = mid + dot(active, down_ref[...])
    normed_out = (final * norm_scale(final) * gout_ref[...]).astype(BF16)
    stats = dot(normed_out, out_ref[...])
    return latent * jnp.exp(stats[:, patch:]) + stats[:, :patch]


def start_copies(sources, targets, sems):
    copies = [pltpu.make_async_copy(s, t, sems.at[i]) for i, (s, t) in enumerate(zip(sources, targets))]
    for copy in copies:
        copy.start()
    return copies


def attend_both(ids, query, own, oth, s_ref, p_ref, pass_heads):
    even = ids[0] == 0
    half = query.shape[1] // 2
    left, right = query[:, :half], query[:, half:]
    own = own()
    own_starts = [(ids[4 + 2 * j], ids[5 + 2 * j]) for j in range(len(own))]
    oth_starts = [(b, a) for a, b in own_starts]
    att_own = attend_half(pick(even, left, right), own, own_starts, ids[1], s_ref, p_ref, pass_heads)
    att_oth = attend_half(pick(even, right, left), oth(), oth_starts, ids[1], s_ref, p_ref, pass_heads)
    return jnp.concatenate([pick(even, att_own, att_oth), pick(even, att_oth, att_own)], axis=1)


def first_step(count, pass_heads, *refs):
    (ids, h_ref, q_ref, z_ref, pos_ref, poshalo_ref, gmlp_ref, gout_ref, win_ref), refs = refs[:9], refs[9:]
    own, refs = refs[:count], refs[count:]
    oth, refs = refs[:count], refs[count:]
    weights, refs = refs[:4], refs[4:]
    pay_ref, s_ref, p_ref = refs[:3]
    held, sems = refs[3:7], refs[7]
    copies = start_copies(weights, held, sems)
    rows = h_ref.shape[0]
    attended = attend_both(ids, q_ref[...], lambda: own, lambda: oth, s_ref, p_ref, pass_heads)
    for copy in copies:
        copy.wait()
    mix_ref, up_ref, down_ref, out_ref = held
    latent = z_ref[...]
    state = finish_step(h_ref[...], attended, latent, mix_ref, gmlp_ref, up_ref, down_ref, gout_ref, out_ref)
    old, new = latent.astype(BF16), state.astype(BF16)
    place = shifted_up(pos_ref[...].astype(F32), poshalo_ref[...].astype(F32))
    old_scale = norm_scale(dot(old, win_ref[...]) + place)
    new_scale = norm_scale(dot(new, win_ref[...]) + place)
    change = new_scale * (new.astype(F32) - old.astype(F32))
    row = lax.broadcasted_iota(jnp.int32, (rows, 1), 0)
    wraps = (row == rows - 1) & (ids[3] == 1)
    change = jnp.where(wraps, 0.0, change)
    ratio = jnp.where(wraps, 1.0, new_scale / old_scale)
    new_scale = jnp.where(wraps, 1.0, new_scale)

    def high_low(value):
        high = value.astype(BF16)
        return high, (value - high.astype(F32)).astype(BF16)

    pay_ref[:, : latent.shape[1]] = change.astype(BF16)
    tail = jnp.zeros((rows, pay_ref.shape[1] - latent.shape[1]), F32)
    lane = lax.broadcasted_iota(jnp.int32, tail.shape, 1)
    for k, value in enumerate((*high_low(ratio), *high_low(new_scale))):
        tail = jnp.where(lane == k, value.astype(F32), tail)
    pay_ref[:, latent.shape[1] :] = tail.astype(BF16)


def second_step(count, pass_heads, *refs):
    (ids, pay_ref, z_ref, halo_ref, pos_ref, gattn_ref, gmlp_ref, gout_ref, win_ref, wq_ref, a_ref), refs = refs[:11], refs[11:]
    own, refs = refs[:count], refs[count:]
    oth, refs = refs[:count], refs[count:]
    weights, refs = refs[:4], refs[4:]
    next_ref, s_ref, p_ref = refs[:3]
    held, sems, wide_ref, kv_ref = refs[3:7], refs[7], refs[8], refs[9]
    copies = start_copies(weights, held, sems)
    rows, patch = z_ref.shape
    total = pay_ref.shape[0]
    for first in range(0, total, rows):
        before = (first - 16) % total
        edge = pay_ref[before : before + 16, :].astype(F32)[15:16]
        wide_ref[first : first + rows, :] = shifted_down(pay_ref[first : first + rows, :].astype(F32), edge)

    mine = wide_ref[pl.ds(pl.multiple_of(ids[1], rows), rows), :]
    old = shifted_down(z_ref[...], halo_ref[...].astype(F32)).astype(BF16).astype(F32)
    new = (old + mine[:, :patch] / (mine[:, patch + 2 : patch + 3] + mine[:, patch + 3 : patch + 4])).astype(BF16)
    hidden = dot(new, win_ref[...]) + pos_ref[...].astype(F32)
    normed = (hidden * norm_scale(hidden) * gattn_ref[...]).astype(BF16)
    scale = (wq_ref.shape[1] // HEADS) ** (-0.5)
    query = (dot(normed, wq_ref[...]).astype(BF16) * scale).astype(BF16)

    half = a_ref.shape[1] // 2

    def renewed(pieces, columns, flipped):
        for j in range(count):
            for part in range(2):
                block = wide_ref[pl.ds(pl.multiple_of(ids[4 + 2 * j + part], rows), rows), :]
                ratio = block[:, patch : patch + 1] + block[:, patch + 1 : patch + 2]
                moved = dot(block[:, :patch].astype(BF16), a_ref[:, columns])
                here = pl.ds((1 - part if flipped else part) * rows, rows)
                kv_ref[j, here, :] = (ratio * pieces[j][here, :].astype(F32) + moved).astype(BF16)
        return [kv_ref.at[j] for j in range(count)]

    attended = attend_both(
        ids,
        query,
        lambda: renewed(own, slice(0, half), False),
        lambda: renewed(oth, slice(half, 2 * half), True),
        s_ref,
        p_ref,
        pass_heads,
    )
    for copy in copies:
        copy.wait()
    mix_ref, up_ref, down_ref, out_ref = held
    next_ref[...] = finish_step(hidden, attended, z_ref[...], mix_ref, gmlp_ref, up_ref, down_ref, gout_ref, out_ref)


def per_device(z, pos, win, gattn, wq, wk, wv, mix, gmlp, up, down, gout, out):
    n = lax.axis_size("seq")
    chips = n // 2
    me = lax.axis_index("seq")
    core, chip = me % 2, me // 2
    rows, patch = z.shape
    half = wq.shape[1] // 2
    order = list(range(0, chips, 2)) + list(range(1, chips, 2))[::-1]
    place_of = [order.index(k) for k in range(chips)]
    forward = [(2 * order[k] + c, 2 * order[(k + 1) % chips] + c) for k in range(chips) for c in range(2)]
    backward = [(b, a) for a, b in forward]
    swap = [(i, i ^ 1) for i in range(n)]
    place = jnp.asarray(place_of, jnp.int32)[chip]
    ring_chip = jnp.asarray(order, jnp.int32)[(place - jnp.arange(chips, dtype=jnp.int32)) % chips]
    blocks = jnp.stack([2 * ring_chip + core, 2 * ring_chip + 1 - core], axis=1).reshape(-1) * rows
    last = (me == n - 1).astype(jnp.int32)
    ids = jnp.concatenate([jnp.stack([core, me * rows, chip, last]).astype(jnp.int32), blocks.astype(jnp.int32)])

    gattn2, gmlp2, gout2 = (g.reshape(1, -1) for g in (gattn, gmlp, gout))
    halo = lax.ppermute(z[-1:].astype(BF16), "seq", [(i, i + 1) for i in range(n - 1)])
    pos_halo = lax.ppermute(pos[:1], "seq", [(i, (i - 1) % n) for i in range(n)])

    shape = jax.ShapeDtypeStruct
    hidden, query, own, oth = pl.pallas_call(
        prologue,
        out_shape=[
            shape((rows, win.shape[1]), F32),
            shape((rows, 2 * half), BF16),
            shape((rows, 2 * half), BF16),
            shape((rows, 2 * half), BF16),
        ],
        in_specs=[SM] + [VM] * 8,
        out_specs=[VM] * 4,
        name="prologue",
    )(ids, z, halo, pos, win, gattn2, wq, wk, wv)

    received = lax.ppermute(oth, "seq", swap)
    held = [None] * chips
    held[0] = jnp.concatenate([own, received], axis=0)
    up_going = down_going = held[0]
    for step in range(1, chips // 2 + 1):
        up_going = lax.ppermute(up_going, "seq", forward)
        held[step] = up_going
        if step < chips - chips // 2:
            down_going = lax.ppermute(down_going, "seq", backward)
            held[chips - step] = down_going
    other = [lax.ppermute(piece, "seq", swap) for piece in held]

    a_map = pl.pallas_call(
        change_map,
        out_shape=shape((patch, 4 * half), BF16),
        in_specs=[SM] + [VM] * 4,
        out_specs=VM,
        cost_estimate=pl.CostEstimate(flops=8 * patch * win.shape[1] * half, bytes_accessed=2**21, transcendentals=0),
        name="change_map",
    )(ids, win, gattn2, wk, wv)

    pass_heads = GROUP if n * rows <= 4096 else 1
    keys = n * rows
    score_scratch = [pltpu.VMEM((pass_heads * rows, keys), F32), pltpu.VMEM((pass_heads * rows, keys), BF16)]
    weights = (mix, up, down, out)
    weight_scratch = [pltpu.VMEM(w.shape, w.dtype) for w in weights] + [pltpu.SemaphoreType.DMA((4,))]
    pay_width = 200
    payload = pl.pallas_call(
        functools.partial(first_step, chips, pass_heads),
        out_shape=shape((rows, pay_width), BF16),
        in_specs=[SM] + [VM] * (8 + 2 * chips) + [HB] * 4,
        out_specs=VM,
        scratch_shapes=score_scratch + weight_scratch,
        name="first_step",
    )(ids, hidden, query, z, pos, pos_halo, gmlp2, gout2, win, *held, *other, *weights)
    gathered = lax.all_gather(payload, "seq", axis=0, tiled=True)
    state = pl.pallas_call(
        functools.partial(second_step, chips, pass_heads),
        out_shape=shape((rows, patch), F32),
        in_specs=[SM] + [VM] * (10 + 2 * chips) + [HB] * 4,
        out_specs=VM,
        scratch_shapes=score_scratch
        + weight_scratch
        + [
            pltpu.VMEM((keys, pay_width), F32),
            pltpu.VMEM((chips, 2 * rows, 2 * half), BF16),
        ],
        name="second_step",
    )(ids, gathered, z, halo, pos, gattn2, gmlp2, gout2, win, wq, a_map, *held, *other, *weights)
    return lax.ppermute(state[::-1], "seq", [(i, n - 1 - i) for i in range(n)])


def solution(mesh):
    token = P(("groups", "seq"), None)
    in_specs = (token, P("seq", None)) + (P(),) * 11
    return jax.shard_map(per_device, mesh=mesh, in_specs=in_specs, out_specs=token, check_vma=False)
```
